32 devices in a mesh: intra: 4 (over y, x), inter: 8 (over z, core).
Axes of the slice: x: 2, y: 2, z: 4, core: 2. Of those that a mesh axis runs over, the one named last changes fastest.
Arguments:
- acts: bfloat16 [4096, 4096], P(('intra', 'inter')), may hold values from -6 to 6
- grad_out: bfloat16 [4096, 512], P(('intra', 'inter')), may hold values from -6 to 6
- codes: int32 [4096, 512], P('intra'), may hold values from -127 to 127
- scales: float32 [2048], P('intra'), may hold values from 0.0002 to 0.0008
Outputs:
- grad_in: bfloat16 [4096, 4096], P(('intra', 'inter'))
- grad_w: float32 [4096, 512], P(('intra', 'inter'))
The draws below stay inside these ranges and needn't reach their ends.
All inputs are finite; a program needn't handle non-finite values.
Results may differ from the reference program's by a relative error of at most 0.0049.
Values may be sent and summed in bfloat16 or wider, within the bound.
A program may use at most 64 MiB of HBM per device.

```python
import math
import jax
import jax.numpy as jnp
from jax import lax

D = 4096
KV = 512
TOKENS = 4096


def set_ends(entries, stream_key, low, largest):
    dims = entries.shape
    index_at = [jax.random.randint(jax.random.fold_in(stream_key, axis), (), 0, dims[axis]) for axis in range(len(dims))]
    entries = entries.at[tuple(index_at)].set(low)
    longest = dims.index(max(dims))
    index_at[longest] = (index_at[longest] + 1) % dims[longest]
    return entries.at[tuple(index_at)].set(largest)


def with_spikes(drawn, own_key, source, target, shards_of, factor):
    owner, partner = [(jnp.arange(drawn.shape[position]) // (drawn.shape[position] // shards_of)).reshape([-1 if axis == position else 1 for axis in range(drawn.ndim)]) for position in (source, target)]
    chosen = jax.random.permutation(own_key, shards_of)[partner]
    strong = (owner == chosen) | (owner == (partner + shards_of // 2) % shards_of)
    return jnp.where(strong, factor * drawn, drawn)


def steps_of(key, extent, shards, low, high):
    gain = 1.0
    for dim, blocks in shards:
        draws = jax.random.uniform(jax.random.fold_in(jax.random.fold_in(key, 6), dim), (blocks,), jnp.float32, low / len(shards), high / len(shards))
        gain = gain * jnp.repeat(jnp.exp(draws), extent[dim] // blocks).reshape((-1,) + (1,) * (len(extent) - 1 - dim))
    return gain


def normal_values(stream_key, extent, width, limit, split=(), kind=jnp.bfloat16):
    array = jax.random.normal(stream_key, extent, jnp.float32) * width
    if len(split) > 0:
        array = steps_of(stream_key, extent, split, -0.22, 0.18) * array
    return jnp.clip(array, min=-limit, max=limit).astype(kind)


def noise_with(stream_key, shape, width, bound, shards, heavy, held_as=jnp.bfloat16):
    drawn = width * jax.random.normal(stream_key, shape, jnp.float32)
    if shards:
        drawn = drawn * steps_of(stream_key, shape, shards, -0.22, 0.18)
    return jnp.clip(with_spikes(drawn, jax.random.fold_in(stream_key, 3), *heavy), -bound, bound).astype(held_as)


def setup_inputs(seed: int = 0) -> dict:
    key_of = jax.random.split(jax.random.key(seed), 5)
    return {
        "acts": noise_with(key_of[0], (TOKENS, D), 1.0, 6.0, ((0, 32),), (0, 1, 32, 2.75)),
        "grad_out": normal_values(key_of[1], (TOKENS, KV), 1.0, 6.0, ((0, 32),)),
        "codes": set_ends(jax.random.randint(key_of[2], (D, KV), -127, 128), jax.random.fold_in(key_of[2], 1), -127, 127).astype(jnp.int32),
        "scales": jnp.clip(jnp.exp(math.log(0.0008) - 1.3862944 * jax.random.uniform(key_of[3], (D // 2,), jnp.float32) ** steps_of(key_of[3], (D // 2,), ((0, 4),), -0.2, 0.2)), 0.0002, 0.0008),
    }


def reference(acts, grad_out, codes, scales):
    blocks = codes.astype(jnp.float32).reshape(D // 2, 2 * KV) * scales[:, None]
    weight = blocks.reshape(D, KV).astype(jnp.bfloat16)
    grad_in = jnp.dot(grad_out, weight.T, preferred_element_type=jnp.float32).astype(jnp.bfloat16)
    summed = lax.dot_general(acts, grad_out, (((0,), (0,)), ((), ())), preferred_element_type=jnp.float32)
    grad_w = summed * jnp.float32(1.0 / math.sqrt(TOKENS))
    return (grad_in, grad_w)
```

```python
import functools
import math

import jax
import jax.numpy as jnp
from jax import lax
from jax.experimental import pallas as pl
from jax.experimental.pallas import tpu as pltpu
from jax.sharding import PartitionSpec as P

MESH = pl.DeviceIdType.MESH


def flip(index, mask, extent):
    out = 0
    bit = 1
    while bit < extent:
        digit = lax.rem(index // bit, 2)
        out = out + bit * (1 - digit if mask & bit else digit)
        bit *= 2
    return out


def kernel(
    ni, nj, acts, go, codes, scales, gin, gw,
    go_all, acts_v, codes_v, scale_v, code_b, ac, pieces, part, rs,
    load_sem, go_send, go_recv, fw_send, a_send, a_recv, p_send, p_recv, r_send, r_recv,
):
    tok, width = acts.shape
    kv = go.shape[1]
    rows = codes.shape[0]
    half = rows // 2
    nz = nj // 2
    blk = rows // nj
    i = lax.axis_index("intra")
    j = lax.axis_index("inter")
    z = j // 2
    c = lax.rem(j, 2)
    oc = 1 - c
    me = 2 * i + c
    far = sorted(range(1, ni), key=lambda d: -bin(d).count("1"))
    near = far[::-1]
    peers = {d: flip(i, d, ni) for d in range(ni)}
    cores = (c, oc)

    def dev(ii, zz, cc):
        return {"intra": ii, "inter": 2 * zz + cc}

    def rdma(src, dst, s, r, where):
        return pltpu.make_async_remote_copy(
            src_ref=src, dst_ref=dst, send_sem=s, recv_sem=r, device_id=where, device_id_type=MESH
        )

    def go_slot(m):
        return go_all.at[pl.ds(pl.multiple_of(m * tok, tok), tok)]

    half_start = pl.multiple_of(c * half, half)
    load_go = pltpu.make_async_copy(go, go_slot(me), load_sem.at[0])
    load_go.start()
    load_acts = pltpu.make_async_copy(acts, acts_v, load_sem.at[1])
    load_acts.start()
    load_codes = pltpu.make_async_copy(codes.at[pl.ds(half_start, half)], codes_v, load_sem.at[2])
    load_codes.start()
    sc_start = pl.multiple_of(c * (half // 2), half // 2)
    load_scale = pltpu.make_async_copy(scales.at[:, pl.ds(sc_start, half // 2)], scale_v, load_sem.at[3])
    load_scale.start()

    barrier = pltpu.get_barrier_semaphore()
    count = 0
    for d in range(ni):
        for k, cc in enumerate(cores):
            if d or k:
                pl.semaphore_signal(barrier, inc=1, device_id=dev(peers[d], z, cc), device_id_type=MESH)
                count += 1
    for k in range(1, nz):
        pl.semaphore_signal(barrier, inc=1, device_id=dev(i, lax.rem(z + k, nz), c), device_id_type=MESH)
        count += 1
    pl.semaphore_wait(barrier, count)

    sends = []

    load_go.wait()
    for d in far + [0]:
        cc = c if d else oc
        cp = rdma(go_slot(me), go_slot(me), go_send.at[d], go_recv.at[me], dev(peers[d], z, cc))
        cp.start()
        sends.append(cp)

    load_acts.wait()
    order = [lax.rem(z + k, nz) for k in range(1, nz)] + [z]

    def ac_slot(h, m):
        return ac.at[h, pl.ds(pl.multiple_of(m * tok, tok), tok)]

    own = []
    for h in order:
        for d in far + [0]:
            for k, cc in enumerate(cores):
                ii = peers[d]
                col = pl.multiple_of(ii * rows + (2 * h + cc) * blk, blk)
                src = acts_v.at[:, pl.ds(col, blk)]
                if d or k:
                    m = 2 * ii + cc
                    cp = rdma(src, ac_slot(h, me), a_send.at[m, h], a_recv.at[me, h], dev(ii, z, cc))
                    sends.append(cp)
                else:
                    cp = pltpu.make_async_copy(src, ac_slot(h, me), a_recv.at[me, h])
                    own.append(cp)
                cp.start()

    load_codes.wait()
    code_b[...] = codes_v[...].astype(jnp.float32).astype(jnp.bfloat16)
    load_scale.wait()
    pick = (
        lax.broadcasted_iota(jnp.int32, (half // 2, half), 1) // 2
        == lax.broadcasted_iota(jnp.int32, (half // 2, half), 0)
    ).astype(jnp.float32).astype(jnp.bfloat16)
    rest = jnp.broadcast_to(scale_v[...], (16, half // 2))
    row_scale = jnp.zeros((16, half), jnp.float32)
    for _ in range(3):
        top = rest.astype(jnp.bfloat16)
        row_scale = row_scale + jnp.dot(top, pick, preferred_element_type=jnp.float32)
        rest = rest - top.astype(jnp.float32)
    row_scale = row_scale[0:1]

    def wait_go(m):
        rdma(go_slot(m), go_slot(m), go_send.at[0], go_recv.at[m], dev(i, z, oc)).wait_recv()

    for d in near:
        m = 2 * peers[d] + c
        wait_go(m)
        cp = rdma(go_slot(m), go_slot(m), fw_send.at[d], go_recv.at[m], dev(i, z, oc))
        cp.start()
        sends.append(cp)

    my_cols = pl.ds(pl.multiple_of(i * rows + c * half, half), half)
    for d in near + [0]:
        ii = peers[d]
        wait_go(2 * ii + oc)
        pair = go_all[pl.ds(pl.multiple_of(2 * ii * tok, 2 * tok), 2 * tok)]
        out = lax.dot_general(
            pair, code_b[...], (((1,), (1,)), ((), ())), preferred_element_type=jnp.float32
        )
        pieces[ii] = (out * row_scale).astype(jnp.bfloat16)
        for k, cc in enumerate(cores):
            m = 2 * ii + cc
            src = pieces.at[ii, pl.ds(pl.multiple_of(cc * tok, tok), tok)]
            if d or k:
                cp = rdma(src, gin.at[:, my_cols], p_send.at[m], p_recv.at[me], dev(ii, z, cc))
                sends.append(cp)
            else:
                cp = pltpu.make_async_copy(src, gin.at[:, my_cols], p_recv.at[me])
                own_piece = cp
            cp.start()

    cot = go_all
    mine = None
    for n, h in enumerate(order):
        own[n].wait()
        for d in range(ni):
            for k, cc in enumerate(cores):
                if d or k:
                    m = 2 * peers[d] + cc
                    rdma(ac_slot(h, m), ac_slot(h, m), a_send.at[m, h], a_recv.at[m, h], dev(i, z, oc)).wait_recv()
        term = lax.dot_general(
            ac[h], cot[...], (((0,), (0,)), ((), ())), preferred_element_type=jnp.float32
        )
        if n < nz - 1:
            part[n] = term.astype(jnp.bfloat16)
            cp = rdma(part.at[n], rs.at[z], r_send.at[n], r_recv.at[z], dev(i, h, c))
            cp.start()
            sends.append(cp)
        else:
            mine = term
    for k in range(1, nz):
        h = lax.rem(z + k, nz)
        rdma(rs.at[h], rs.at[h], r_send.at[0], r_recv.at[h], dev(i, h, c)).wait_recv()
        mine = mine + rs[h].astype(jnp.float32)
    gw[...] = mine * (1.0 / math.sqrt(tok * ni * nj))

    own_piece.wait()
    for d in range(ni):
        for k, cc in enumerate(cores):
            if d or k:
                ii = peers[d]
                m = 2 * ii + cc
                cols = pl.ds(pl.multiple_of(ii * rows + cc * half, half), half)
                rdma(gin.at[:, cols], gin.at[:, cols], p_send.at[m], p_recv.at[m], dev(i, z, oc)).wait_recv()
    for cp in sends:
        cp.wait_send()


def fused(ni, nj, acts, grad_out, codes, scales):
    tok, width = acts.shape
    kv = grad_out.shape[1]
    rows = codes.shape[0]
    half, nz, blk = rows // 2, nj // 2, rows // nj
    group = 2 * ni
    dma = pltpu.SemaphoreType.DMA
    bf16 = jnp.bfloat16
    anyspace = pl.BlockSpec(memory_space=pl.ANY)
    return tuple(pl.pallas_call(
        functools.partial(kernel, ni, nj),
        out_shape=(
            jax.ShapeDtypeStruct((tok, width), bf16),
            jax.ShapeDtypeStruct((blk, kv), jnp.float32),
        ),
        in_specs=[anyspace] * 4,
        out_specs=(anyspace, pl.BlockSpec(memory_space=pltpu.VMEM)),
        scratch_shapes=[
            pltpu.VMEM((group * tok, kv), bf16),
            pltpu.VMEM((tok, width), bf16),
            pltpu.VMEM((half, kv), jnp.int32),
            pltpu.VMEM((1, half // 2), jnp.float32),
            pltpu.VMEM((half, kv), bf16),
            pltpu.VMEM((nz, group * tok, blk), bf16),
            pltpu.VMEM((ni, 2 * tok, half), bf16),
            pltpu.VMEM((max(nz - 1, 1), blk, kv), bf16),
            pltpu.VMEM((nz, blk, kv), bf16),
            dma((4,)),
            dma((ni,)), dma((group,)), dma((ni,)),
            dma((group, nz)), dma((group, nz)),
            dma((group,)), dma((group,)),
            dma((nz,)), dma((nz,)),
        ],
        compiler_params=pltpu.CompilerParams(collective_id=0, has_side_effects=True),
    )(acts, grad_out, codes, scales.reshape(1, -1)))


def plain(acts, grad_out, codes, scales):
    rows = codes.shape[0]
    width_kv = codes.shape[1]
    blocks = codes.astype(jnp.float32).reshape(rows // 2, 2 * width_kv) * scales[:, None]
    local_weight = blocks.reshape(rows, width_kv).astype(jnp.bfloat16)
    n_group = lax.axis_size("intra")
    n_cross = lax.axis_size("inter")
    factor = 1.0 / math.sqrt(acts.shape[0] * n_group * n_cross)
    contract = (((0,), (0,)), ((), ()))
    group_cot = lax.all_gather(grad_out, "intra", axis=0, tiled=True)
    columns_owned = lax.all_to_all(acts, "intra", split_axis=1, concat_axis=0, tiled=True)
    grad_w = lax.psum_scatter(
        lax.dot_general(columns_owned, group_cot, contract, preferred_element_type=jnp.float32)
        * factor,
        "inter",
        scatter_dimension=0,
        tiled=True,
    )
    pieces = jnp.dot(group_cot, local_weight.T, preferred_element_type=jnp.float32).astype(
        jnp.bfloat16
    )
    grad_in = lax.all_to_all(pieces, "intra", split_axis=0, concat_axis=1, tiled=True)
    return (grad_in, grad_w)


def solution(mesh):
    ni, nj = mesh.shape["intra"], mesh.shape["inter"]

    def per_device(acts, grad_out, codes, scales):
        rows = codes.shape[0]
        aligned = rows % (nj * 128) == 0 and rows % 512 == 0 and acts.shape[0] % 16 == 0
        if aligned and nj % 2 == 0 and ni & (ni - 1) == 0 and acts.shape[1] == ni * rows:
            return fused(ni, nj, acts, grad_out, codes, scales)
        return plain(acts, grad_out, codes, scales)

    in_specs = (
        P(("intra", "inter"), None),
        P(("intra", "inter"), None),
        P("intra", None),
        P("intra"),
    )
    out_specs = (P(("intra", "inter"), None), P(("intra", "inter"), None))
    return jax.shard_map(
        per_device, mesh=mesh, in_specs=in_specs, out_specs=out_specs, check_vma=False
    )
```

```python
import functools
import math

import jax
import jax.numpy as jnp
from jax import lax
from jax.experimental import pallas as pl
from jax.experimental.pallas import tpu as pltpu
from jax.sharding import PartitionSpec as P

MESH = pl.DeviceIdType.MESH


def flip(index, mask, extent):
    out = 0
    bit = 1
    while bit < extent:
        digit = lax.rem(index // bit, 2)
        out = out + bit * (1 - digit if mask & bit else digit)
        bit *= 2
    return out


def lane_scale(scale_row, half):
    pick = (
        lax.broadcasted_iota(jnp.int32, (half // 2, half), 1) // 2
        == lax.broadcasted_iota(jnp.int32, (half // 2, half), 0)
    ).astype(jnp.float32).astype(jnp.bfloat16)
    rest = jnp.broadcast_to(scale_row, (16, half // 2))
    total = jnp.zeros((16, half), jnp.float32)
    for _ in range(3):
        top = rest.astype(jnp.bfloat16)
        total = total + jnp.dot(top, pick, preferred_element_type=jnp.float32)
        rest = rest - top.astype(jnp.float32)
    return total[0:1]


def kernel(
    ni, nj, acts, go, codes, scales, gin, gw,
    go_all, acts_v, codes_v, scale_v, scale_d, code_b, code_d, ac, pieces, part, rs,
    load_sem, go_send, go_recv, gh_send, gh_recv, fw_send, a_send, a_recv, p_send, p_recv,
    r_send, r_recv, s_sem, w_sem, up_send, down_send, w_recv,
):
    tok, width = acts.shape
    rows = codes.shape[0]
    half = rows // 2
    nz = nj // 2
    blk = rows // nj
    quarter = half // nz
    i = lax.axis_index("intra")
    j = lax.axis_index("inter")
    z = j // 2
    c = lax.rem(j, 2)
    oc = 1 - c
    me = 2 * i + c
    peers = {d: flip(i, d, ni) for d in range(ni)}
    near, diag = (1, 2), 3
    cores = (c, oc)

    def dev(ii, zz, cc):
        return {"intra": ii, "inter": 2 * zz + cc}

    def rdma(src, dst, s, r, where):
        return pltpu.make_async_remote_copy(
            src_ref=src, dst_ref=dst, send_sem=s, recv_sem=r, device_id=where, device_id_type=MESH
        )

    def arrived(ref, s, r):
        rdma(ref, ref, s, r, dev(i, z, oc)).wait_recv()

    sends = []

    def send(*args):
        cp = rdma(*args)
        cp.start()
        sends.append(cp)

    def go_slot(m):
        return go_all.at[pl.ds(pl.multiple_of(m * tok, tok), tok)]

    def go_half(m, n):
        return go_all.at[pl.ds(pl.multiple_of(m * tok + n * (tok // 2), tok // 2), tok // 2)]

    def ac_slot(h, m):
        return ac.at[h, pl.ds(pl.multiple_of(m * tok, tok), tok)]

    def cols_of(ii, cc):
        return pl.ds(pl.multiple_of(ii * rows + cc * half, half), half)

    half_start = pl.multiple_of(c * half, half)
    sc_start = pl.multiple_of(c * (half // 2), half // 2)
    load_codes = pltpu.make_async_copy(codes.at[pl.ds(half_start, half)], codes_v, load_sem.at[2])
    load_codes.start()
    load_scale = pltpu.make_async_copy(scales.at[:, pl.ds(sc_start, half // 2)], scale_v, load_sem.at[3])
    load_scale.start()
    load_go = pltpu.make_async_copy(go, go_slot(me), load_sem.at[0])
    load_go.start()
    load_acts = pltpu.make_async_copy(acts, acts_v, load_sem.at[1])
    load_acts.start()

    barrier = pltpu.get_barrier_semaphore()
    count = 0
    for d in range(ni):
        for k, cc in enumerate(cores):
            if d or k:
                pl.semaphore_signal(barrier, inc=1, device_id=dev(peers[d], z, cc), device_id_type=MESH)
                count += 1
    for k in range(1, nz):
        pl.semaphore_signal(barrier, inc=1, device_id=dev(i, lax.rem(z + k, nz), c), device_id_type=MESH)
        count += 1

    load_codes.wait()
    code_b[...] = codes_v[...].astype(jnp.float32).astype(jnp.bfloat16)
    load_go.wait()
    load_scale.wait()
    pl.semaphore_wait(barrier, count)

    for d in near:
        send(go_slot(me), go_slot(me), go_send.at[d], go_recv.at[me], dev(peers[d], z, c))
    send(go_slot(me), go_slot(me), go_send.at[0], go_recv.at[me], dev(i, z, oc))

    def slice_of(ref, q):
        return ref.at[pl.ds(pl.multiple_of(q * quarter, quarter), quarter)]

    send(slice_of(code_b, z), slice_of(code_d, z), w_sem.at[0], w_recv.at[z], dev(peers[diag], z, c))
    send(scale_v, scale_d, s_sem.at[0], s_sem.at[1], dev(peers[diag], z, c))

    load_acts.wait()
    order = [lax.rem(z + k, nz) for k in range(1, nz)] + [z]
    own = []

    def send_columns(h):
        for d in (diag,) + near + (0,):
            for k, cc in enumerate(cores):
                ii = peers[d]
                col = pl.multiple_of(ii * rows + (2 * h + cc) * blk, blk)
                src = acts_v.at[:, pl.ds(col, blk)]
                if d or k:
                    m = 2 * ii + cc
                    send(src, ac_slot(h, me), a_send.at[m, h], a_recv.at[me, h], dev(ii, z, cc))
                else:
                    cp = pltpu.make_async_copy(src, ac_slot(h, me), a_recv.at[me, h])
                    cp.start()
                    own.append(cp)

    send_columns(order[0])
    row_scale = lane_scale(scale_v[...], half)

    def wait_go(m):
        arrived(go_slot(m), go_send.at[0], go_recv.at[m])

    for n, d in enumerate(near):
        m = 2 * peers[d] + c
        wait_go(m)
        send(go_half(m, n), go_half(m, n), gh_send.at[n], gh_recv.at[n], dev(peers[diag ^ d], z, c))
        send(go_slot(m), go_slot(m), fw_send.at[d], go_recv.at[m], dev(i, z, oc))
    for h in order[1:]:
        send_columns(h)

    def pass_on(q, up):
        where = z + 1 if up else z - 1
        sem = up_send if up else down_send
        return rdma(slice_of(code_d, q), slice_of(code_d, q), sem.at[q], w_recv.at[q], dev(i, where, c))

    def may_pass(up):
        return z + 1 < nz if up else z >= 1

    def has(step, up):
        return z - step >= 0 if up else z + step < nz

    arrived(slice_of(code_d, z), w_sem.at[0], w_recv.at[z])
    for up in (True, False):
        @pl.when(may_pass(up))
        def _():
            pass_on(z, up).start()

    def relay(step):
        for up in (True, False):
            @pl.when(has(step, up))
            def _():
                q = z - step if up else z + step
                arrived(slice_of(code_d, q), w_sem.at[0], w_recv.at[q])

                @pl.when(may_pass(up))
                def _():
                    pass_on(q, up).start()

    def pieces_of(ii, code, scale):
        pair = go_all[pl.ds(pl.multiple_of(2 * ii * tok, 2 * tok), 2 * tok)]
        out = lax.dot_general(
            pair, code[...], (((1,), (1,)), ((), ())), preferred_element_type=jnp.float32
        )
        return (out * scale).astype(jnp.bfloat16)

    def piece(n, cc):
        return pieces.at[n, pl.ds(pl.multiple_of(cc * tok, tok), tok)]

    for d in near:
        ii = peers[d]
        wait_go(2 * ii + oc)
        pieces[d] = pieces_of(ii, code_b, row_scale)
        for cc in cores:
            m = 2 * ii + cc
            send(piece(d, cc), gin.at[:, cols_of(i, c)], p_send.at[m], p_recv.at[me], dev(ii, z, cc))
    wait_go(2 * i + oc)
    pieces[0] = pieces_of(i, code_b, row_scale)
    send(piece(0, oc), gin.at[:, cols_of(i, c)], p_send.at[2 * i + oc], p_recv.at[me], dev(i, z, oc))
    keep = pltpu.make_async_copy(piece(0, c), gin.at[:, cols_of(i, c)], p_recv.at[me])
    keep.start()

    m = 2 * peers[diag] + c
    for n in range(2):
        arrived(go_half(m, n), gh_send.at[n], gh_recv.at[n])
    send(go_slot(m), go_slot(m), fw_send.at[diag], go_recv.at[m], dev(i, z, oc))
    wait_go(2 * peers[diag] + oc)

    mine = None
    for n, h in enumerate(order):
        own[n].wait()
        for d in range(ni):
            for k, cc in enumerate(cores):
                if d or k:
                    m = 2 * peers[d] + cc
                    arrived(ac_slot(h, m), a_send.at[m, h], a_recv.at[m, h])
        term = lax.dot_general(
            ac[h], go_all[...], (((0,), (0,)), ((), ())), preferred_element_type=jnp.float32
        )
        if n < nz - 1:
            part[n] = term.astype(jnp.bfloat16)
            send(part.at[n], rs.at[z], r_send.at[n], r_recv.at[z], dev(i, h, c))
            relay(n + 1)
        else:
            mine = term

    arrived(scale_d, s_sem.at[0], s_sem.at[1])
    dd = peers[diag]
    pieces[diag] = pieces_of(i, code_d, lane_scale(scale_d[...], half))
    send(piece(diag, oc), gin.at[:, cols_of(dd, c)], p_send.at[2 * dd + c], p_recv.at[2 * dd + c], dev(i, z, oc))
    keep_d = pltpu.make_async_copy(piece(diag, c), gin.at[:, cols_of(dd, c)], load_sem.at[4])
    keep_d.start()

    for k in range(1, nz):
        h = lax.rem(z + k, nz)
        arrived(rs.at[h], r_send.at[0], r_recv.at[h])
        mine = mine + rs[h].astype(jnp.float32)
    gw[...] = mine * (1.0 / math.sqrt(tok * ni * nj))

    keep.wait()
    keep_d.wait()
    for d in range(ni):
        for k, cc in enumerate(cores):
            if (d != diag and (d or k)) or (d == diag and k):
                ii = peers[d]
                block = gin.at[:, cols_of(ii, cc)]
                arrived(block, p_send.at[2 * ii + cc], p_recv.at[2 * ii + cc])
    for cp in sends:
        cp.wait_send()
    for step in range(nz):
        for up in (True, False):
            @pl.when(jnp.logical_and(has(step, up), may_pass(up)))
            def _():
                pass_on(z - step if up else z + step, up).wait_send()


def fused(ni, nj, acts, grad_out, codes, scales):
    tok, width = acts.shape
    kv = grad_out.shape[1]
    rows = codes.shape[0]
    half, nz, blk = rows // 2, nj // 2, rows // nj
    group = 2 * ni
    dma = pltpu.SemaphoreType.DMA
    bf16 = jnp.bfloat16
    anyspace = pl.BlockSpec(memory_space=pl.ANY)
    return tuple(pl.pallas_call(
        functools.partial(kernel, ni, nj),
        out_shape=(
            pltpu.VMEM((tok, width), bf16),
            pltpu.VMEM((blk, kv), jnp.float32),
        ),
        in_specs=[anyspace] * 4,
        out_specs=(pl.BlockSpec(memory_space=pltpu.VMEM),) * 2,
        scratch_shapes=[
            pltpu.VMEM((group * tok, kv), bf16),
            pltpu.VMEM((tok, width), bf16),
            pltpu.VMEM((half, kv), jnp.int32),
            pltpu.VMEM((1, half // 2), jnp.float32),
            pltpu.VMEM((1, half // 2), jnp.float32),
            pltpu.VMEM((half, kv), bf16),
            pltpu.VMEM((half, kv), bf16),
            pltpu.VMEM((nz, group * tok, blk), bf16),
            pltpu.VMEM((ni, 2 * tok, half), bf16),
            pltpu.VMEM((max(nz - 1, 1), blk, kv), bf16),
            pltpu.VMEM((nz, blk, kv), bf16),
            dma((5,)),
            dma((ni,)), dma((group,)), dma((2,)), dma((2,)), dma((ni,)),
            dma((group, nz)), dma((group, nz)),
            dma((group,)), dma((group,)),
            dma((nz,)), dma((nz,)),
            dma((2,)), dma((1,)), dma((nz,)), dma((nz,)), dma((nz,)),
        ],
        compiler_params=pltpu.CompilerParams(collective_id=0, has_side_effects=True),
    )(acts, grad_out, codes, scales.reshape(1, -1)))


def plain(acts, grad_out, codes, scales):
    rows = codes.shape[0]
    width_kv = codes.shape[1]
    blocks = codes.astype(jnp.float32).reshape(rows // 2, 2 * width_kv) * scales[:, None]
    local_weight = blocks.reshape(rows, width_kv).astype(jnp.bfloat16)
    n_group = lax.axis_size("intra")
    n_cross = lax.axis_size("inter")
    factor = 1.0 / math.sqrt(acts.shape[0] * n_group * n_cross)
    contract = (((0,), (0,)), ((), ()))
    group_cot = lax.all_gather(grad_out, "intra", axis=0, tiled=True)
    columns_owned = lax.all_to_all(acts, "intra", split_axis=1, concat_axis=0, tiled=True)
    grad_w = lax.psum_scatter(
        lax.dot_general(columns_owned, group_cot, contract, preferred_element_type=jnp.float32)
        * factor,
        "inter",
        scatter_dimension=0,
        tiled=True,
    )
    pieces = jnp.dot(group_cot, local_weight.T, preferred_element_type=jnp.float32).astype(
        jnp.bfloat16
    )
    grad_in = lax.all_to_all(pieces, "intra", split_axis=0, concat_axis=1, tiled=True)
    return (grad_in, grad_w)


def solution(mesh):
    ni, nj = mesh.shape["intra"], mesh.shape["inter"]

    def per_device(acts, grad_out, codes, scales):
        rows = codes.shape[0]
        aligned = rows % (nj * 128) == 0 and rows % 512 == 0 and acts.shape[0] % 16 == 0
        if aligned and nj % 2 == 0 and ni == 4 and acts.shape[1] == ni * rows:
            return fused(ni, nj, acts, grad_out, codes, scales)
        return plain(acts, grad_out, codes, scales)

    in_specs = (
        P(("intra", "inter"), None),
        P(("intra", "inter"), None),
        P("intra", None),
        P("intra"),
    )
    out_specs = (P(("intra", "inter"), None), P(("intra", "inter"), None))
    return jax.shard_map(
        per_device, mesh=mesh, in_specs=in_specs, out_specs=out_specs, check_vma=False
    )
```

```python
import functools
import math

import jax
import jax.numpy as jnp
from jax import lax
from jax.experimental import pallas as pl
from jax.experimental.pallas import tpu as pltpu
from jax.sharding import PartitionSpec as P

MESH = pl.DeviceIdType.MESH


def flip(index, mask, extent):
    out = 0
    bit = 1
    while bit < extent:
        digit = lax.rem(index // bit, 2)
        out = out + bit * (1 - digit if mask & bit else digit)
        bit *= 2
    return out


def lane_scale(scale_row, half):
    pick = (
        lax.broadcasted_iota(jnp.int32, (half // 2, half), 1) // 2
        == lax.broadcasted_iota(jnp.int32, (half // 2, half), 0)
    ).astype(jnp.float32).astype(jnp.bfloat16)
    rest = jnp.broadcast_to(scale_row, (16, half // 2))
    total = jnp.zeros((16, half), jnp.float32)
    for _ in range(3):
        top = rest.astype(jnp.bfloat16)
        total = total + jnp.dot(top, pick, preferred_element_type=jnp.float32)
        rest = rest - top.astype(jnp.float32)
    return total[0:1]


def kernel(
    ni, nj, acts, go, codes, scales, gin, gw,
    go_all, acts_v, codes_v, scale_v, code_b, ac, pieces, part, rs,
    load_sem, go_send, go_recv, gh_send, gh_recv, fw_send, a_send, a_recv, p_send, p_recv,
    r_send, r_recv,
):
    tok, width = acts.shape
    rows = codes.shape[0]
    half = rows // 2
    nz = nj // 2
    blk = rows // nj
    i = lax.axis_index("intra")
    j = lax.axis_index("inter")
    z = j // 2
    c = lax.rem(j, 2)
    oc = 1 - c
    me = 2 * i + c
    peers = {d: flip(i, d, ni) for d in range(ni)}
    near, diag = (1, 2), 3
    cores = (c, oc)

    def dev(ii, zz, cc):
        return {"intra": ii, "inter": 2 * zz + cc}

    def rdma(src, dst, s, r, where):
        return pltpu.make_async_remote_copy(
            src_ref=src, dst_ref=dst, send_sem=s, recv_sem=r, device_id=where, device_id_type=MESH
        )

    def arrived(ref, s, r):
        rdma(ref, ref, s, r, dev(i, z, oc)).wait_recv()

    sends = []

    def send(*args):
        cp = rdma(*args)
        cp.start()
        sends.append(cp)

    def go_slot(m):
        return go_all.at[pl.ds(pl.multiple_of(m * tok, tok), tok)]

    def go_half(m, n):
        return go_all.at[pl.ds(pl.multiple_of(m * tok + n * (tok // 2), tok // 2), tok // 2)]

    def ac_slot(h, m):
        return ac.at[h, pl.ds(pl.multiple_of(m * tok, tok), tok)]

    def cols_of(ii, cc):
        return pl.ds(pl.multiple_of(ii * rows + cc * half, half), half)

    half_start = pl.multiple_of(c * half, half)
    sc_start = pl.multiple_of(c * (half // 2), half // 2)
    load_codes = pltpu.make_async_copy(codes.at[pl.ds(half_start, half)], codes_v, load_sem.at[2])
    load_codes.start()
    load_scale = pltpu.make_async_copy(scales.at[:, pl.ds(sc_start, half // 2)], scale_v, load_sem.at[3])
    load_scale.start()
    load_go = pltpu.make_async_copy(go, go_slot(me), load_sem.at[0])
    load_go.start()
    load_acts = pltpu.make_async_copy(acts, acts_v, load_sem.at[1])
    load_acts.start()

    barrier = pltpu.get_barrier_semaphore()
    count = 0
    for d in range(ni):
        for k, cc in enumerate(cores):
            if d or k:
                pl.semaphore_signal(barrier, inc=1, device_id=dev(peers[d], z, cc), device_id_type=MESH)
                count += 1
    for k in range(1, nz):
        pl.semaphore_signal(barrier, inc=1, device_id=dev(i, lax.rem(z + k, nz), c), device_id_type=MESH)
        count += 1

    load_codes.wait()
    code_b[...] = codes_v[...].astype(jnp.float32).astype(jnp.bfloat16)
    load_go.wait()
    load_scale.wait()
    pl.semaphore_wait(barrier, count)

    for d in near:
        send(go_slot(me), go_slot(me), go_send.at[d], go_recv.at[me], dev(peers[d], z, c))
    send(go_slot(me), go_slot(me), go_send.at[0], go_recv.at[me], dev(i, z, oc))

    load_acts.wait()
    order = [lax.rem(z + k, nz) for k in range(1, nz)] + [z]
    own = []

    def send_columns(h):
        for d in (diag,) + near + (0,):
            for k, cc in enumerate(cores):
                ii = peers[d]
                col = pl.multiple_of(ii * rows + (2 * h + cc) * blk, blk)
                src = acts_v.at[:, pl.ds(col, blk)]
                if d or k:
                    m = 2 * ii + cc
                    send(src, ac_slot(h, me), a_send.at[m, h], a_recv.at[me, h], dev(ii, z, cc))
                else:
                    cp = pltpu.make_async_copy(src, ac_slot(h, me), a_recv.at[me, h])
                    cp.start()
                    own.append(cp)

    send_columns(order[0])
    row_scale = lane_scale(scale_v[...], half)

    def wait_go(m):
        arrived(go_slot(m), go_send.at[0], go_recv.at[m])

    for n, d in enumerate(near):
        m = 2 * peers[d] + c
        wait_go(m)
        send(go_half(m, n), go_half(m, n), gh_send.at[n], gh_recv.at[n], dev(peers[diag ^ d], z, c))
        send(go_slot(m), go_slot(m), fw_send.at[d], go_recv.at[m], dev(i, z, oc))
    for h in order[1:]:
        send_columns(h)

    def pieces_of(ii, code, scale):
        pair = go_all[pl.ds(pl.multiple_of(2 * ii * tok, 2 * tok), 2 * tok)]
        out = lax.dot_general(
            pair, code[...], (((1,), (1,)), ((), ())), preferred_element_type=jnp.float32
        )
        return (out * scale).astype(jnp.bfloat16)

    def piece(n, cc):
        return pieces.at[n, pl.ds(pl.multiple_of(cc * tok, tok), tok)]

    for d in near:
        ii = peers[d]
        wait_go(2 * ii + oc)
        pieces[d] = pieces_of(ii, code_b, row_scale)
        for cc in cores:
            m = 2 * ii + cc
            send(piece(d, cc), gin.at[:, cols_of(i, c)], p_send.at[m], p_recv.at[me], dev(ii, z, cc))
    wait_go(2 * i + oc)
    pieces[0] = pieces_of(i, code_b, row_scale)
    send(piece(0, oc), gin.at[:, cols_of(i, c)], p_send.at[2 * i + oc], p_recv.at[me], dev(i, z, oc))
    keep = pltpu.make_async_copy(piece(0, c), gin.at[:, cols_of(i, c)], p_recv.at[me])
    keep.start()

    m = 2 * peers[diag] + c
    for n in range(2):
        arrived(go_half(m, n), gh_send.at[n], gh_recv.at[n])
    send(go_slot(m), go_slot(m), fw_send.at[diag], go_recv.at[m], dev(i, z, oc))
    wait_go(2 * peers[diag] + oc)
    dd = peers[diag]
    pieces[diag] = pieces_of(dd, code_b, row_scale)
    for cc in cores:
        m = 2 * dd + cc
        send(piece(diag, cc), gin.at[:, cols_of(i, c)], p_send.at[m], p_recv.at[me], dev(dd, z, cc))

    mine = None
    for n, h in enumerate(order):
        own[n].wait()
        for d in range(ni):
            for k, cc in enumerate(cores):
                if d or k:
                    m = 2 * peers[d] + cc
                    arrived(ac_slot(h, m), a_send.at[m, h], a_recv.at[m, h])
        term = lax.dot_general(
            ac[h], go_all[...], (((0,), (0,)), ((), ())), preferred_element_type=jnp.float32
        )
        if n < nz - 1:
            part[n] = term.astype(jnp.bfloat16)
            send(part.at[n], rs.at[z], r_send.at[n], r_recv.at[z], dev(i, h, c))
        else:
            mine = term

    for k in range(1, nz):
        h = lax.rem(z + k, nz)
        arrived(rs.at[h], r_send.at[0], r_recv.at[h])
        mine = mine + rs[h].astype(jnp.float32)
    gw[...] = mine * (1.0 / math.sqrt(tok * ni * nj))

    keep.wait()
    for d in range(ni):
        for k, cc in enumerate(cores):
            if d or k:
                ii = peers[d]
                block = gin.at[:, cols_of(ii, cc)]
                arrived(block, p_send.at[2 * ii + cc], p_recv.at[2 * ii + cc])
    for cp in sends:
        cp.wait_send()


def fused(ni, nj, acts, grad_out, codes, scales):
    tok, width = acts.shape
    kv = grad_out.shape[1]
    rows = codes.shape[0]
    half, nz, blk = rows // 2, nj // 2, rows // nj
    group = 2 * ni
    dma = pltpu.SemaphoreType.DMA
    bf16 = jnp.bfloat16
    anyspace = pl.BlockSpec(memory_space=pl.ANY)
    return tuple(pl.pallas_call(
        functools.partial(kernel, ni, nj),
        out_shape=(
            pltpu.VMEM((tok, width), bf16),
            pltpu.VMEM((blk, kv), jnp.float32),
        ),
        in_specs=[anyspace] * 4,
        out_specs=(pl.BlockSpec(memory_space=pltpu.VMEM),) * 2,
        scratch_shapes=[
            pltpu.VMEM((group * tok, kv), bf16),
            pltpu.VMEM((tok, width), bf16),
            pltpu.VMEM((half, kv), jnp.int32),
            pltpu.VMEM((1, half // 2), jnp.float32),
            pltpu.VMEM((half, kv), bf16),
            pltpu.VMEM((nz, group * tok, blk), bf16),
            pltpu.VMEM((ni, 2 * tok, half), bf16),
            pltpu.VMEM((max(nz - 1, 1), blk, kv), bf16),
            pltpu.VMEM((nz, blk, kv), bf16),
            dma((4,)),
            dma((ni,)), dma((group,)), dma((2,)), dma((2,)), dma((ni,)),
            dma((group, nz)), dma((group, nz)),
            dma((group,)), dma((group,)),
            dma((nz,)), dma((nz,)),
        ],
        compiler_params=pltpu.CompilerParams(collective_id=0, has_side_effects=True),
    )(acts, grad_out, codes, scales.reshape(1, -1)))


def plain(acts, grad_out, codes, scales):
    rows = codes.shape[0]
    width_kv = codes.shape[1]
    blocks = codes.astype(jnp.float32).reshape(rows // 2, 2 * width_kv) * scales[:, None]
    local_weight = blocks.reshape(rows, width_kv).astype(jnp.bfloat16)
    n_group = lax.axis_size("intra")
    n_cross = lax.axis_size("inter")
    factor = 1.0 / math.sqrt(acts.shape[0] * n_group * n_cross)
    contract = (((0,), (0,)), ((), ()))
    group_cot = lax.all_gather(grad_out, "intra", axis=0, tiled=True)
    columns_owned = lax.all_to_all(acts, "intra", split_axis=1, concat_axis=0, tiled=True)
    grad_w = lax.psum_scatter(
        lax.dot_general(columns_owned, group_cot, contract, preferred_element_type=jnp.float32)
        * factor,
        "inter",
        scatter_dimension=0,
        tiled=True,
    )
    pieces = jnp.dot(group_cot, local_weight.T, preferred_element_type=jnp.float32).astype(
        jnp.bfloat16
    )
    grad_in = lax.all_to_all(pieces, "intra", split_axis=0, concat_axis=1, tiled=True)
    return (grad_in, grad_w)


def solution(mesh):
    ni, nj = mesh.shape["intra"], mesh.shape["inter"]

    def per_device(acts, grad_out, codes, scales):
        rows = codes.shape[0]
        aligned = rows % (nj * 128) == 0 and rows % 512 == 0 and acts.shape[0] % 16 == 0
        if aligned and nj % 2 == 0 and ni == 4 and acts.shape[1] == ni * rows:
            return fused(ni, nj, acts, grad_out, codes, scales)
        return plain(acts, grad_out, codes, scales)

    in_specs = (
        P(("intra", "inter"), None),
        P(("intra", "inter"), None),
        P("intra", None),
        P("intra"),
    )
    out_specs = (P(("intra", "inter"), None), P(("intra", "inter"), None))
    return jax.shard_map(
        per_device, mesh=mesh, in_specs=in_specs, out_specs=out_specs, check_vma=False
    )
```

```python
import functools
import math

import jax
import jax.numpy as jnp
from jax import lax
from jax.experimental import pallas as pl
from jax.experimental.pallas import tpu as pltpu
from jax.sharding import PartitionSpec as P

MESH = pl.DeviceIdType.MESH


def flip(index, mask, extent):
    out = 0
    bit = 1
    while bit < extent:
        digit = lax.rem(index // bit, 2)
        out = out + bit * (1 - digit if mask & bit else digit)
        bit *= 2
    return out


def lane_scale(scale_row, half):
    pick = (
        lax.broadcasted_iota(jnp.int32, (half // 2, half), 1) // 2
        == lax.broadcasted_iota(jnp.int32, (half // 2, half), 0)
    ).astype(jnp.float32).astype(jnp.bfloat16)
    rest = jnp.broadcast_to(scale_row, (16, half // 2))
    total = jnp.zeros((16, half), jnp.float32)
    for _ in range(3):
        top = rest.astype(jnp.bfloat16)
        total = total + jnp.dot(top, pick, preferred_element_type=jnp.float32)
        rest = rest - top.astype(jnp.float32)
    return total[0:1]


def kernel(
    ni, nj, acts, go, codes, scales, gin, gw,
    go_all, acts_v, codes_v, scale_v, code_b, ac, pieces, part, rs,
    load_sem, go_send, go_recv, gh_send, gh_recv, fw_send, a_send, a_recv, p_send, p_recv,
    r_send, r_recv,
):
    tok, width = acts.shape
    rows = codes.shape[0]
    half = rows // 2
    nz = nj // 2
    blk = rows // nj
    i = lax.axis_index("intra")
    j = lax.axis_index("inter")
    z = j // 2
    c = lax.rem(j, 2)
    oc = 1 - c
    me = 2 * i + c
    peers = {d: flip(i, d, ni) for d in range(ni)}
    near, diag = (1, 2), 3
    cores = (c, oc)

    def dev(ii, zz, cc):
        return {"intra": ii, "inter": 2 * zz + cc}

    def rdma(src, dst, s, r, where):
        return pltpu.make_async_remote_copy(
            src_ref=src, dst_ref=dst, send_sem=s, recv_sem=r, device_id=where, device_id_type=MESH
        )

    def arrived(ref, s, r):
        rdma(ref, ref, s, r, dev(i, z, oc)).wait_recv()

    sends = []

    def send(*args):
        cp = rdma(*args)
        cp.start()
        sends.append(cp)

    def go_slot(m):
        return go_all.at[pl.ds(pl.multiple_of(m * tok, tok), tok)]

    def go_half(m, n):
        return go_all.at[pl.ds(pl.multiple_of(m * tok + n * (tok // 2), tok // 2), tok // 2)]

    def ac_slot(h, m):
        return ac.at[h, pl.ds(pl.multiple_of(m * tok, tok), tok)]

    def cols_of(ii, cc):
        return pl.ds(pl.multiple_of(ii * rows + cc * half, half), half)

    half_start = pl.multiple_of(c * half, half)
    sc_start = pl.multiple_of(c * (half // 2), half // 2)
    load_go = pltpu.make_async_copy(go, go_slot(me), load_sem.at[0])
    load_go.start()
    load_acts = pltpu.make_async_copy(acts, acts_v, load_sem.at[1])
    load_acts.start()

    load_codes = pltpu.make_async_copy(codes.at[pl.ds(half_start, half)], codes_v, load_sem.at[2])
    load_codes.start()
    load_scale = pltpu.make_async_copy(scales.at[:, pl.ds(sc_start, half // 2)], scale_v, load_sem.at[3])
    load_scale.start()
    barrier = pltpu.get_barrier_semaphore()
    count = 0
    for d in range(ni):
        for k, cc in enumerate(cores):
            if d or k:
                pl.semaphore_signal(barrier, inc=1, device_id=dev(peers[d], z, cc), device_id_type=MESH)
                count += 1
    for k in range(1, nz):
        pl.semaphore_signal(barrier, inc=1, device_id=dev(i, lax.rem(z + k, nz), c), device_id_type=MESH)
        count += 1

    load_go.wait()
    pl.semaphore_wait(barrier, count)

    for d in near:
        send(go_slot(me), go_slot(me), go_send.at[d], go_recv.at[me], dev(peers[d], z, c))
    send(go_slot(me), go_slot(me), go_send.at[0], go_recv.at[me], dev(i, z, oc))

    load_acts.wait()
    order = [lax.rem(z + k, nz) for k in range(1, nz)] + [z]
    own = []

    def send_columns(h):
        for d in near + (0, diag):
            for k, cc in enumerate(cores):
                ii = peers[d]
                col = pl.multiple_of(ii * rows + (2 * h + cc) * blk, blk)
                src = acts_v.at[:, pl.ds(col, blk)]
                if d or k:
                    m = 2 * ii + cc
                    send(src, ac_slot(h, me), a_send.at[m, h], a_recv.at[me, h], dev(ii, z, cc))
                else:
                    cp = pltpu.make_async_copy(src, ac_slot(h, me), a_recv.at[me, h])
                    cp.start()
                    own.append(cp)

    send_columns(order[0])
    load_codes.wait()
    code_b[...] = codes_v[...].astype(jnp.float32).astype(jnp.bfloat16)
    load_scale.wait()
    row_scale = lane_scale(scale_v[...], half)

    def wait_go(m):
        arrived(go_slot(m), go_send.at[0], go_recv.at[m])

    for n, d in enumerate(near):
        m = 2 * peers[d] + c
        wait_go(m)
        send(go_half(m, n), go_half(m, n), gh_send.at[n], gh_recv.at[n], dev(peers[diag ^ d], z, c))
        send(go_slot(m), go_slot(m), fw_send.at[d], go_recv.at[m], dev(i, z, oc))
    for h in order[1:]:
        send_columns(h)

    def pieces_of(ii, code, scale):
        pair = go_all[pl.ds(pl.multiple_of(2 * ii * tok, 2 * tok), 2 * tok)]
        out = lax.dot_general(
            pair, code[...], (((1,), (1,)), ((), ())), preferred_element_type=jnp.float32
        )
        return (out * scale).astype(jnp.bfloat16)

    def piece(n, cc):
        return pieces.at[n, pl.ds(pl.multiple_of(cc * tok, tok), tok)]

    for d in near:
        ii = peers[d]
        wait_go(2 * ii + oc)
        pieces[d] = pieces_of(ii, code_b, row_scale)
        for cc in cores:
            m = 2 * ii + cc
            send(piece(d, cc), gin.at[:, cols_of(i, c)], p_send.at[m], p_recv.at[me], dev(ii, z, cc))
    wait_go(2 * i + oc)
    pieces[0] = pieces_of(i, code_b, row_scale)
    send(piece(0, oc), gin.at[:, cols_of(i, c)], p_send.at[2 * i + oc], p_recv.at[me], dev(i, z, oc))
    keep = pltpu.make_async_copy(piece(0, c), gin.at[:, cols_of(i, c)], p_recv.at[me])
    keep.start()

    m = 2 * peers[diag] + c
    for n in range(2):
        arrived(go_half(m, n), gh_send.at[n], gh_recv.at[n])
    send(go_slot(m), go_slot(m), fw_send.at[diag], go_recv.at[m], dev(i, z, oc))
    wait_go(2 * peers[diag] + oc)
    dd = peers[diag]
    pieces[diag] = pieces_of(dd, code_b, row_scale)
    for cc in cores:
        m = 2 * dd + cc
        send(piece(diag, cc), gin.at[:, cols_of(i, c)], p_send.at[m], p_recv.at[me], dev(dd, z, cc))

    mine = None
    for n, h in enumerate(order):
        own[n].wait()
        for d in range(ni):
            for k, cc in enumerate(cores):
                if d or k:
                    m = 2 * peers[d] + cc
                    arrived(ac_slot(h, m), a_send.at[m, h], a_recv.at[m, h])
        term = lax.dot_general(
            ac[h], go_all[...], (((0,), (0,)), ((), ())), preferred_element_type=jnp.float32
        )
        if n < nz - 1:
            part[n] = term.astype(jnp.bfloat16)
            send(part.at[n], rs.at[z], r_send.at[n], r_recv.at[z], dev(i, h, c))
        else:
            mine = term

    for k in range(1, nz):
        h = lax.rem(z + k, nz)
        arrived(rs.at[h], r_send.at[0], r_recv.at[h])
        mine = mine + rs[h].astype(jnp.float32)
    gw[...] = mine * (1.0 / math.sqrt(tok * ni * nj))

    keep.wait()
    for d in range(ni):
        for k, cc in enumerate(cores):
            if d or k:
                ii = peers[d]
                block = gin.at[:, cols_of(ii, cc)]
                arrived(block, p_send.at[2 * ii + cc], p_recv.at[2 * ii + cc])
    for cp in sends:
        cp.wait_send()


def fused(ni, nj, acts, grad_out, codes, scales):
    tok, width = acts.shape
    kv = grad_out.shape[1]
    rows = codes.shape[0]
    half, nz, blk = rows // 2, nj // 2, rows // nj
    group = 2 * ni
    dma = pltpu.SemaphoreType.DMA
    bf16 = jnp.bfloat16
    anyspace = pl.BlockSpec(memory_space=pl.ANY)
    return tuple(pl.pallas_call(
        functools.partial(kernel, ni, nj),
        out_shape=(
            pltpu.VMEM((tok, width), bf16),
            pltpu.VMEM((blk, kv), jnp.float32),
        ),
        in_specs=[anyspace] * 4,
        out_specs=(pl.BlockSpec(memory_space=pltpu.VMEM),) * 2,
        scratch_shapes=[
            pltpu.VMEM((group * tok, kv), bf16),
            pltpu.VMEM((tok, width), bf16),
            pltpu.VMEM((half, kv), jnp.int32),
            pltpu.VMEM((1, half // 2), jnp.float32),
            pltpu.VMEM((half, kv), bf16),
            pltpu.VMEM((nz, group * tok, blk), bf16),
            pltpu.VMEM((ni, 2 * tok, half), bf16),
            pltpu.VMEM((max(nz - 1, 1), blk, kv), bf16),
            pltpu.VMEM((nz, blk, kv), bf16),
            dma((4,)),
            dma((ni,)), dma((group,)), dma((2,)), dma((2,)), dma((ni,)),
            dma((group, nz)), dma((group, nz)),
            dma((group,)), dma((group,)),
            dma((nz,)), dma((nz,)),
        ],
        compiler_params=pltpu.CompilerParams(collective_id=0, has_side_effects=True),
    )(acts, grad_out, codes, scales.reshape(1, -1)))


def plain(acts, grad_out, codes, scales):
    rows = codes.shape[0]
    width_kv = codes.shape[1]
    blocks = codes.astype(jnp.float32).reshape(rows // 2, 2 * width_kv) * scales[:, None]
    local_weight = blocks.reshape(rows, width_kv).astype(jnp.bfloat16)
    n_group = lax.axis_size("intra")
    n_cross = lax.axis_size("inter")
    factor = 1.0 / math.sqrt(acts.shape[0] * n_group * n_cross)
    contract = (((0,), (0,)), ((), ()))
    group_cot = lax.all_gather(grad_out, "intra", axis=0, tiled=True)
    columns_owned = lax.all_to_all(acts, "intra", split_axis=1, concat_axis=0, tiled=True)
    grad_w = lax.psum_scatter(
        lax.dot_general(columns_owned, group_cot, contract, preferred_element_type=jnp.float32)
        * factor,
        "inter",
        scatter_dimension=0,
        tiled=True,
    )
    pieces = jnp.dot(group_cot, local_weight.T, preferred_element_type=jnp.float32).astype(
        jnp.bfloat16
    )
    grad_in = lax.all_to_all(pieces, "intra", split_axis=0, concat_axis=1, tiled=True)
    return (grad_in, grad_w)


def solution(mesh):
    ni, nj = mesh.shape["intra"], mesh.shape["inter"]

    def per_device(acts, grad_out, codes, scales):
        rows = codes.shape[0]
        aligned = rows % (nj * 128) == 0 and rows % 512 == 0 and acts.shape[0] % 16 == 0
        if aligned and nj % 2 == 0 and ni == 4 and acts.shape[1] == ni * rows:
            return fused(ni, nj, acts, grad_out, codes, scales)
        return plain(acts, grad_out, codes, scales)

    in_specs = (
        P(("intra", "inter"), None),
        P(("intra", "inter"), None),
        P("intra", None),
        P("intra"),
    )
    out_specs = (P(("intra", "inter"), None), P(("intra", "inter"), None))
    return jax.shard_map(
        per_device, mesh=mesh, in_specs=in_specs, out_specs=out_specs, check_vma=False
    )
```
